32 devices in a mesh: data: 1 (over z), wg: 32 (over y, x, core).
Axes of the slice: x: 4, y: 4, z: 1, core: 2. Of those that a mesh axis runs over, the one named last changes fastest.
The devices are a block of a 4x4x8 slice.
Arguments:
- hidden: bfloat16 [32, 512, 1600], P(('data', 'wg'))
- k_cache: bfloat16 [3, 32, 256, 25, 64], P(None, ('data', 'wg'))
- v_cache: bfloat16 [3, 32, 256, 25, 64], P(None, ('data', 'wg'))
- attn_gain: float32 [3, 1600], replicated
- attn_shift: float32 [3, 1600], replicated
- qkv_weight: bfloat16 [3, 1600, 3, 25, 64], P(None, 'wg')
- qkv_bias: float32 [3, 3, 25, 64], replicated
- out_weight: bfloat16 [3, 25, 64, 1600], P(None, None, None, 'wg')
- out_bias: float32 [3, 1600], replicated
- mlp_gain: float32 [3, 1600], replicated
- mlp_shift: float32 [3, 1600], replicated
- up_weight: bfloat16 [3, 1600, 6400], P(None, 'wg')
- up_bias: float32 [3, 6400], replicated
- down_weight: bfloat16 [3, 6400, 1600], P(None, None, 'wg')
- down_bias: float32 [3, 1600], replicated
- final_gain: float32 [1600], replicated
- final_shift: float32 [1600], replicated
Outputs:
- output 1: bfloat16 [32, 512, 1600], P(('data', 'wg'))
- output 2: bfloat16 [3, 32, 512, 25, 64], P(None, ('data', 'wg'))
- output 3: bfloat16 [3, 32, 512, 25, 64], P(None, ('data', 'wg'))
All inputs are finite; a program needn't handle non-finite values.
Results may differ from the reference program's by a relative error of at most 0.0141109.
Values are sent between devices in bfloat16 or wider.
A program may use at most 768 MiB of HBM per device.

```python
import jax
import jax.numpy as jnp
from jax import lax

NUM_SEQS = 32
NEW_TOKENS = 512
PREFIX_LEN = 256
NUM_LAYERS = 3
MODEL_DIM = 1600
FFN_DIM = 6400
NUM_HEADS = 25
HEAD_DIM = 64


def setup_inputs(seed: int = 0, part: int = 0) -> dict:
    part_key = jax.random.fold_in(jax.random.key(seed), part)
    act_keys = jax.random.split(part_key, 3)
    shared = jax.random.split(jax.random.key(seed + 1), 14)
    inner_dim = NUM_HEADS * HEAD_DIM
    layers = NUM_LAYERS

    def normal(rng_key, array_shape, spread):
        return jax.random.normal(rng_key, array_shape, jnp.float32) * spread

    cache_shape = (layers, NUM_SEQS, PREFIX_LEN, NUM_HEADS, HEAD_DIM)
    return {
        "hidden": normal(act_keys[0], (NUM_SEQS, NEW_TOKENS, MODEL_DIM), 1.0).astype(jnp.bfloat16),
        "k_cache": normal(act_keys[1], cache_shape, 1.0).astype(jnp.bfloat16),
        "v_cache": normal(act_keys[2], cache_shape, 1.0).astype(jnp.bfloat16),
        "attn_gain": 1.0 + normal(shared[0], (layers, MODEL_DIM), 0.3),
        "attn_shift": normal(shared[1], (layers, MODEL_DIM), 0.3),
        "qkv_weight": normal(shared[2], (layers, MODEL_DIM, 3, NUM_HEADS, HEAD_DIM), MODEL_DIM ** -0.5).astype(jnp.bfloat16),
        "qkv_bias": normal(shared[3], (layers, 3, NUM_HEADS, HEAD_DIM), 0.5),
        "out_weight": normal(shared[4], (layers, NUM_HEADS, HEAD_DIM, MODEL_DIM), inner_dim ** -0.5).astype(jnp.bfloat16),
        "out_bias": normal(shared[5], (layers, MODEL_DIM), 0.5),
        "mlp_gain": 1.0 + normal(shared[6], (layers, MODEL_DIM), 0.3),
        "mlp_shift": normal(shared[7], (layers, MODEL_DIM), 0.3),
        "up_weight": normal(shared[8], (layers, MODEL_DIM, FFN_DIM), MODEL_DIM ** -0.5).astype(jnp.bfloat16),
        "up_bias": normal(shared[9], (layers, FFN_DIM), 0.5),
        "down_weight": normal(shared[10], (layers, FFN_DIM, MODEL_DIM), FFN_DIM ** -0.5).astype(jnp.bfloat16),
        "down_bias": normal(shared[11], (layers, MODEL_DIM), 0.5),
        "final_gain": 1.0 + normal(shared[12], (MODEL_DIM,), 0.3),
        "final_shift": normal(shared[13], (MODEL_DIM,), 0.3),
    }


def layer_norm(values, gain, shift):
    widened = values.astype(jnp.float32)
    mean_val = jnp.mean(widened, axis=-1, keepdims=True)
    centered = widened - mean_val
    variance = jnp.mean(centered * centered, axis=-1, keepdims=True)
    return centered * lax.rsqrt(variance + 1e-5) * gain + shift


def attend_sequence(operands):
    query, keys_all, values_all = operands
    new_len = query.shape[0]
    total_len = keys_all.shape[0]
    scores = jnp.einsum("thk,shk->hts", query.astype(jnp.float32), keys_all.astype(jnp.float32)) * (HEAD_DIM ** -0.5)
    allowed = jnp.arange(total_len)[None, :] <= jnp.arange(new_len)[:, None] + (total_len - new_len)
    scores = jnp.where(allowed[None], scores, -1e30)
    probs = jax.nn.softmax(scores, axis=-1).astype(jnp.bfloat16)
    attended = jnp.einsum("hts,shk->thk", probs.astype(jnp.float32), values_all.astype(jnp.float32))
    return attended.astype(jnp.bfloat16)


def reference(hidden, k_cache, v_cache, attn_gain, attn_shift, qkv_weight, qkv_bias, out_weight, out_bias, mlp_gain, mlp_shift, up_weight, up_bias, down_weight, down_bias, final_gain, final_shift):
    def one_layer(state, layer_params):
        (a_gain, a_shift, w_qkv, b_qkv, w_out, b_out, m_gain, m_shift, w_up, b_up, w_down, b_down, cache_k, cache_v) = layer_params
        normed = layer_norm(state, a_gain, a_shift).astype(jnp.bfloat16)
        projected = jnp.einsum("btd,dchk->btchk", normed.astype(jnp.float32), w_qkv.astype(jnp.float32)) + b_qkv
        projected = projected.astype(jnp.bfloat16)
        query = projected[:, :, 0]
        key_new = projected[:, :, 1]
        value_new = projected[:, :, 2]
        keys_all = jnp.concatenate([cache_k, key_new], axis=1)
        values_all = jnp.concatenate([cache_v, value_new], axis=1)
        attended = lax.map(attend_sequence, (query, keys_all, values_all))
        attn_out = jnp.einsum("bthk,hkd->btd", attended.astype(jnp.float32), w_out.astype(jnp.float32)) + b_out
        middle = (state.astype(jnp.float32) + attn_out).astype(jnp.bfloat16)
        normed_mlp = layer_norm(middle, m_gain, m_shift).astype(jnp.bfloat16)
        pre_act = jnp.einsum("btd,df->btf", normed_mlp.astype(jnp.float32), w_up.astype(jnp.float32)) + b_up
        activated = jax.nn.gelu(pre_act, approximate=True).astype(jnp.bfloat16)
        down_out = jnp.einsum("btf,fd->btd", activated.astype(jnp.float32), w_down.astype(jnp.float32)) + b_down
        new_state = (middle.astype(jnp.float32) + down_out).astype(jnp.bfloat16)
        return new_state, (key_new, value_new)

    stacked = (attn_gain, attn_shift, qkv_weight, qkv_bias, out_weight, out_bias, mlp_gain, mlp_shift, up_weight, up_bias, down_weight, down_bias, k_cache, v_cache)
    last_state, new_kv = lax.scan(one_layer, hidden, stacked)
    output = layer_norm(last_state, final_gain, final_shift).astype(jnp.bfloat16)
    return (output, new_kv[0], new_kv[1])
```

```python
import functools
import math

import jax
import jax.numpy as jnp
from jax import lax
from jax.experimental import pallas as pl
from jax.experimental.pallas import tpu as pltpu
from jax.sharding import PartitionSpec as P

MESH = pl.DeviceIdType.MESH
LANES = 128


class Torus:
    def __init__(self, axis, side, send_sem, recv_sem, local_sem):
        me = lax.axis_index(axis)
        self.axis, self.side = axis, side
        self.core = lax.rem(me, 2)
        self.x = lax.rem(me // 2, side)
        self.y = me // (2 * side)
        self.send_sem, self.recv_sem, self.local_sem = send_sem, recv_sem, local_sem

    def coord(self, dim, k):
        return lax.rem((self.x if dim == "x" else self.y) + (k + self.side), self.side)

    def device(self, y, x, core):
        return {self.axis: (y * self.side + x) * 2 + core}

    def step(self, dim, k):
        if dim == "x":
            return self.device(self.y, self.coord("x", k), self.core)
        return self.device(self.coord("y", k), self.x, self.core)

    def partner(self):
        return self.device(self.y, self.x, 1 - self.core)

    def meet(self):
        barrier = pltpu.get_barrier_semaphore()
        peers = [self.step(dim, k) for dim in ("x", "y") for k in (1, -1)] + [self.partner()]
        for peer in peers:
            pl.semaphore_signal(barrier, inc=1, device_id=peer, device_id_type=MESH)
        pl.semaphore_wait(barrier, len(peers))


class Unit:
    def __init__(self, torus, index, shard, landing):
        self.torus, self.index, self.shard, self.landing = torus, index, shard, landing
        half = shard.shape[-1] // LANES // 2 * LANES
        self.columns = (pl.ds(0, half), pl.ds(half, shard.shape[-1] - half))
        self.rank = len(shard.shape)
        cut = shard.shape[0] // 2
        self.rows = (slice(None), pl.ds(0, cut), pl.ds(cut, shard.shape[0] - cut))

    def _tail(self, t, part):
        return (self.rows[part],) + (slice(None),) * (self.rank - 2) + (self.columns[t],)

    def own(self, t):
        return self.shard.at[self._tail(t, 0)]

    def piece(self, t, k, part=0):
        torus = self.torus
        where = (torus.y, torus.coord("x", k)) if t == 0 else (torus.coord("y", k), torus.x)
        return self.landing.at[(torus.core,) + where + self._tail(t, part)]

    def block(self, t, k, part=0):
        torus = self.torus
        where = (torus.coord("y", k), slice(None)) if t == 0 else (slice(None), torus.coord("x", k))
        return self.landing.at[(torus.core,) + where + self._tail(t, part)]

    def copy(self, t, slot):
        torus = self.torus
        first, second = ("x", "y") if t == 0 else ("y", "x")
        source, target, device = {
            0: lambda: (self.own(t), self.piece(t, 0), torus.step(first, 1)),
            1: lambda: (self.own(t), self.piece(t, 0), torus.step(first, -1)),
            2: lambda: (self.piece(t, -1, 1), None, torus.step(first, 1)),
            3: lambda: (self.piece(t, 1, 2), None, torus.step(first, -1)),
            4: lambda: (self.block(t, 0), None, torus.step(second, 1)),
            5: lambda: (self.block(t, 0), None, torus.step(second, -1)),
            6: lambda: (self.block(t, -1, 1), None, torus.step(second, 1)),
            7: lambda: (self.block(t, 1, 2), None, torus.step(second, -1)),
            8: lambda: (self.block(t, 0), None, torus.partner()),
            9: lambda: (self.block(t, -1), None, torus.partner()),
            10: lambda: (self.block(t, 1), None, torus.partner()),
            11: lambda: (self.block(t, 2), None, torus.partner()),
        }[slot]()
        return pltpu.make_async_remote_copy(
            src_ref=source, dst_ref=source if target is None else target,
            send_sem=torus.send_sem.at[self.index, t, slot], recv_sem=torus.recv_sem.at[self.index, t, slot],
            device_id=device, device_id_type=MESH)

    def keep(self, t):
        return pltpu.make_async_copy(self.own(t), self.piece(t, 0), self.torus.local_sem.at[self.index, t])

    def start(self, *slots):
        for t in range(2):
            for slot in slots:
                self.copy(t, slot).start()

    def arrived(self, *slots):
        for t in range(2):
            for slot in slots:
                self.copy(t, slot).wait_recv()

    def send_own(self):
        self.start(0, 1)
        for t in range(2):
            self.keep(t).start()

    def relay_own(self):
        self.arrived(0, 1)
        self.start(2, 3)

    def send_block(self):
        for t in range(2):
            self.keep(t).wait()
        self.arrived(2, 3)
        self.start(4, 5, 8)

    def relay_block(self):
        self.arrived(4, 5)
        self.start(6, 7, 9, 10)

    def last_block(self):
        self.arrived(6, 7)
        self.start(11)

    def complete(self):
        self.arrived(8, 9, 10, 11)

    def drain(self):
        for t in range(2):
            for slot in range(12):
                self.copy(t, slot).wait_send()


def gather_kernel(axis, side, shard, extra, landing, landing_extra, send_sem, recv_sem, local_sem):
    torus = Torus(axis, side, send_sem, recv_sem, local_sem)
    torus.meet()
    count = shard.shape[0]
    rest = Unit(torus, count, extra, landing_extra)

    def unit(u):
        return Unit(torus, u, shard.at[u], landing.at[u])

    rest.send_own()
    rest.relay_own()
    unit(0).send_own()
    rest.send_block()
    unit(0).relay_own()
    rest.relay_block()

    def turn(u, carry):
        @pl.when(u + 1 < count)
        def _():
            unit(u + 1).send_own()

        unit(u).send_block()

        @pl.when(u + 1 < count)
        def _():
            unit(u + 1).relay_own()

        @pl.when(u > 0)
        def _():
            unit(u - 1).last_block()
            unit(u - 1).complete()

        unit(u).relay_block()
        return carry

    lax.fori_loop(0, count, turn, 0)
    rest.last_block()
    rest.complete()
    unit(count - 1).last_block()
    unit(count - 1).complete()
    rest.drain()

    def drain(u, carry):
        unit(u).drain()
        return carry

    lax.fori_loop(0, count, drain, 0)


def gather_all(axis, size, shard, extra):
    side = math.isqrt(size // 2)
    count, rows, columns = shard.shape
    return pl.pallas_call(
        functools.partial(gather_kernel, axis, side),
        out_shape=(jax.ShapeDtypeStruct((count, 2, side, side, rows, columns), shard.dtype),
                   jax.ShapeDtypeStruct((2, side, side) + extra.shape, extra.dtype)),
        in_specs=[pl.BlockSpec(memory_space=pltpu.VMEM)] * 2,
        out_specs=(pl.BlockSpec(memory_space=pl.ANY),) * 2,
        scratch_shapes=[pltpu.SemaphoreType.DMA((count + 1, 2, 12)), pltpu.SemaphoreType.DMA((count + 1, 2, 12)),
                        pltpu.SemaphoreType.DMA((count + 1, 2))],
        compiler_params=pltpu.CompilerParams(collective_id=0, has_side_effects=True, vmem_limit_bytes=32 * 2**20),
    )(shard, extra)


def layer_norm(values, gain, shift):
    widened = values.astype(jnp.float32)
    mean_val = jnp.mean(widened, axis=-1, keepdims=True)
    centered = widened - mean_val
    variance = jnp.mean(centered * centered, axis=-1, keepdims=True)
    return centered * lax.rsqrt(variance + 1e-5) * gain + shift


def attention(query, cache_k, cache_v, key_new, value_new):
    new_len = query.shape[1]
    factor = query.shape[-1] ** -0.5
    prefix_scores = jnp.einsum("bthk,bshk->bhts", query, cache_k, preferred_element_type=jnp.float32) * factor
    self_scores = jnp.einsum("bthk,bshk->bhts", query, key_new, preferred_element_type=jnp.float32) * factor
    allowed = jnp.arange(new_len)[None, :] <= jnp.arange(new_len)[:, None]
    self_scores = jnp.where(allowed, self_scores, -1e30)
    row_max = jnp.maximum(jnp.max(prefix_scores, axis=-1, keepdims=True), jnp.max(self_scores, axis=-1, keepdims=True))
    prefix_exp = jnp.exp(prefix_scores - row_max)
    self_exp = jnp.exp(self_scores - row_max)
    denom_sum = jnp.sum(prefix_exp, axis=-1, keepdims=True) + jnp.sum(self_exp, axis=-1, keepdims=True)
    prefix_probs = (prefix_exp / denom_sum).astype(jnp.bfloat16)
    self_probs = (self_exp / denom_sum).astype(jnp.bfloat16)
    attended = jnp.einsum("bhts,bshk->bhtk", prefix_probs, cache_v, preferred_element_type=jnp.float32)
    attended = attended + jnp.einsum("bhts,bshk->bhtk", self_probs, value_new, preferred_element_type=jnp.float32)
    return attended.astype(jnp.bfloat16)


def decoder_layer(state, cache_k, cache_v, attn_gain, attn_shift, w_qkv, b_qkv, w_out, b_out, mlp_gain, mlp_shift, w_up, b_up, w_down, b_down):
    normed = layer_norm(state, attn_gain, attn_shift).astype(jnp.bfloat16)
    projected = (jnp.einsum("btd,dchk->btchk", normed, w_qkv, preferred_element_type=jnp.float32) + b_qkv).astype(jnp.bfloat16)
    query = projected[:, :, 0]
    key_new = projected[:, :, 1]
    value_new = projected[:, :, 2]
    attended = attention(query, cache_k, cache_v, key_new, value_new)
    attn_out = jnp.einsum("bhtk,hkd->btd", attended, w_out, preferred_element_type=jnp.float32) + b_out
    middle = (state.astype(jnp.float32) + attn_out).astype(jnp.bfloat16)
    normed_mlp = layer_norm(middle, mlp_gain, mlp_shift).astype(jnp.bfloat16)
    pre_act = jnp.einsum("btd,df->btf", normed_mlp, w_up, preferred_element_type=jnp.float32) + b_up
    activated = jax.nn.gelu(pre_act, approximate=True).astype(jnp.bfloat16)
    down_out = jnp.einsum("btf,fd->btd", activated, w_down, preferred_element_type=jnp.float32) + b_down
    new_state = (middle.astype(jnp.float32) + down_out).astype(jnp.bfloat16)
    return new_state, key_new, value_new


def solution(mesh):
    part_axis, group_axis = mesh.axis_names
    seq_spec = P((part_axis, group_axis))
    cache_spec = P(None, (part_axis, group_axis))
    replicated = P()
    in_specs = (seq_spec, cache_spec, cache_spec, replicated, replicated, P(None, group_axis), replicated,
                P(None, None, None, group_axis), replicated, replicated, replicated, P(None, group_axis), replicated,
                P(None, None, group_axis), replicated, replicated, replicated)
    out_specs = (seq_spec, cache_spec, cache_spec)

    def local_program(hidden, k_cache, v_cache, attn_gain, attn_shift, qkv_weight, qkv_bias, out_weight, out_bias, mlp_gain, mlp_shift, up_weight, up_bias, down_weight, down_bias, final_gain, final_shift):
        state = hidden
        layers, depth = up_weight.shape[0], up_weight.shape[1]
        inner = out_weight.shape[1] * out_weight.shape[2]
        wide = up_weight.shape[2]
        heads, head_dim = out_weight.shape[1:3]
        model = hidden.shape[-1]
        even = depth // 16 * 16
        w_q = qkv_weight.reshape(layers, depth, 3 * inner)
        w_o = jnp.transpose(out_weight, (0, 3, 1, 2)).reshape(layers, depth, inner)
        w_d = jnp.swapaxes(down_weight, 1, 2)
        shards = jnp.stack([jnp.concatenate([w_q, w_o], axis=2), up_weight, w_d], axis=1)
        shards = shards.reshape(layers * 3, depth, wide)
        main, rest = gather_all(group_axis, mesh.shape[group_axis], shards[:, :even], shards[:, even:])

        def whole(unit):
            a = jnp.transpose(main[unit], (1, 2, 0, 3, 4))
            b = jnp.transpose(rest[:, :, :, unit], (1, 2, 0, 3, 4))
            return jnp.concatenate([a, b], axis=3).reshape(model, wide)

        keys_out = []
        values_out = []
        for layer_idx in range(qkv_weight.shape[0]):
            mixed = whole(3 * layer_idx)
            w_qkv = mixed[:, :3 * inner].reshape(model, 3, heads, head_dim)
            w_out = jnp.transpose(mixed[:, 3 * inner:]).reshape(heads, head_dim, model)
            w_up = whole(3 * layer_idx + 1)
            w_down = jnp.transpose(whole(3 * layer_idx + 2))
            state, key_new, value_new = decoder_layer(
                state, k_cache[layer_idx], v_cache[layer_idx], attn_gain[layer_idx], attn_shift[layer_idx],
                w_qkv, qkv_bias[layer_idx], w_out, out_bias[layer_idx], mlp_gain[layer_idx], mlp_shift[layer_idx],
                w_up, up_bias[layer_idx], w_down, down_bias[layer_idx])
            keys_out.append(key_new)
            values_out.append(value_new)
        output = layer_norm(state, final_gain, final_shift).astype(jnp.bfloat16)
        return output, jnp.stack(keys_out), jnp.stack(values_out)

    return jax.shard_map(local_program, mesh=mesh, in_specs=in_specs, out_specs=out_specs, check_vma=False)
```

```python
import functools
import math

import jax
import jax.numpy as jnp
from jax import lax
from jax.experimental import pallas as pl
from jax.experimental.pallas import tpu as pltpu
from jax.sharding import PartitionSpec as P

MESH = pl.DeviceIdType.MESH
LANES = 128


class Torus:
    def __init__(self, axis, side, send_sem, recv_sem, local_sem):
        me = lax.axis_index(axis)
        self.axis, self.side = axis, side
        self.core = lax.rem(me, 2)
        self.x = lax.rem(me // 2, side)
        self.y = me // (2 * side)
        self.send_sem, self.recv_sem, self.local_sem = send_sem, recv_sem, local_sem

    def coord(self, dim, k):
        return lax.rem((self.x if dim == "x" else self.y) + (k + self.side), self.side)

    def device(self, y, x, core):
        return {self.axis: (y * self.side + x) * 2 + core}

    def step(self, dim, k):
        if dim == "x":
            return self.device(self.y, self.coord("x", k), self.core)
        return self.device(self.coord("y", k), self.x, self.core)

    def partner(self):
        return self.device(self.y, self.x, 1 - self.core)

    def meet(self):
        barrier = pltpu.get_barrier_semaphore()
        peers = [self.step(dim, k) for dim in ("x", "y") for k in (1, -1)] + [self.partner()]
        for peer in peers:
            pl.semaphore_signal(barrier, inc=1, device_id=peer, device_id_type=MESH)
        pl.semaphore_wait(barrier, len(peers))


class Unit:
    def __init__(self, torus, index, shard, landing):
        self.torus, self.index, self.shard, self.landing = torus, index, shard, landing
        half = shard.shape[-1] // LANES // 2 * LANES
        self.columns = (pl.ds(0, half), pl.ds(half, shard.shape[-1] - half))
        self.rank = len(shard.shape)
        cut = shard.shape[0] // 2
        self.rows = (slice(None), pl.ds(0, cut), pl.ds(cut, shard.shape[0] - cut))

    def _tail(self, t, part):
        return (self.rows[part],) + (slice(None),) * (self.rank - 2) + (self.columns[t],)

    def own(self, t):
        return self.shard.at[self._tail(t, 0)]

    def piece(self, t, k, part=0):
        torus = self.torus
        where = (torus.y, torus.coord("x", k)) if t == 0 else (torus.coord("y", k), torus.x)
        return self.landing.at[(torus.core,) + where + self._tail(t, part)]

    def block(self, t, k, part=0):
        torus = self.torus
        where = (torus.coord("y", k), slice(None)) if t == 0 else (slice(None), torus.coord("x", k))
        return self.landing.at[(torus.core,) + where + self._tail(t, part)]

    def copy(self, t, slot):
        torus = self.torus
        first, second = ("x", "y") if t == 0 else ("y", "x")
        source, target, device = {
            0: lambda: (self.own(t), self.piece(t, 0), torus.step(first, 1)),
            1: lambda: (self.own(t), self.piece(t, 0), torus.step(first, -1)),
            2: lambda: (self.piece(t, -1, 1), None, torus.step(first, 1)),
            3: lambda: (self.piece(t, 1, 2), None, torus.step(first, -1)),
            4: lambda: (self.block(t, 0), None, torus.step(second, 1)),
            5: lambda: (self.block(t, 0), None, torus.step(second, -1)),
            6: lambda: (self.block(t, -1, 1), None, torus.step(second, 1)),
            7: lambda: (self.block(t, 1, 2), None, torus.step(second, -1)),
            8: lambda: (self.block(t, 0), None, torus.partner()),
            9: lambda: (self.block(t, -1), None, torus.partner()),
            10: lambda: (self.block(t, 1), None, torus.partner()),
            11: lambda: (self.block(t, 2), None, torus.partner()),
        }[slot]()
        return pltpu.make_async_remote_copy(
            src_ref=source, dst_ref=source if target is None else target,
            send_sem=torus.send_sem.at[self.index, t, slot], recv_sem=torus.recv_sem.at[self.index, t, slot],
            device_id=device, device_id_type=MESH)

    def keep(self, t):
        return pltpu.make_async_copy(self.own(t), self.piece(t, 0), self.torus.local_sem.at[self.index, t])

    def start(self, *slots):
        for t in range(2):
            for slot in slots:
                self.copy(t, slot).start()

    def arrived(self, *slots):
        for t in range(2):
            for slot in slots:
                self.copy(t, slot).wait_recv()

    def send_own(self):
        self.start(0, 1)
        for t in range(2):
            self.keep(t).start()

    def relay_own(self):
        self.arrived(0, 1)
        self.start(2, 3)

    def send_block(self):
        for t in range(2):
            self.keep(t).wait()
        self.arrived(2, 3)
        self.start(4, 5, 8)

    def relay_block(self):
        self.arrived(4, 5)
        self.start(6, 7, 9, 10)

    def last_block(self):
        self.arrived(6, 7)
        self.start(11)

    def complete(self):
        self.arrived(8, 9, 10, 11)

    def drain(self):
        for t in range(2):
            for slot in range(12):
                self.copy(t, slot).wait_send()

TILE = 1280
CHUNK = 256
F32 = jnp.float32
BF16 = jnp.bfloat16


def dot(a, b, dims=((1,), (0,))):
    return lax.dot_general(a, b, (dims, ((), ())), preferred_element_type=F32)


def normalized(block):
    wide = block.astype(F32)
    centered = wide - jnp.mean(wide, axis=0, keepdims=True)
    return centered * lax.rsqrt(jnp.mean(centered * centered, axis=0, keepdims=True) + 1e-5)


def prefill_kernel(axis, side, heads, head_dim, shard, extra, hidden, k_cache, v_cache, gains, qkv_bias, up_bias, sides,
                   out, k_out, v_out, landing, landing_extra,
                   h_t, a_ref, qkv_t, o_t, u_ref, w_rest, w_buf, raw, acc, kc, vc,
                   send_sem, recv_sem, local_sem, w_sem, raw_sem, cache_sem, kv_sem):
    torus = Torus(axis, side, send_sem, recv_sem, local_sem)
    torus.meet()
    count = shard.shape[0]
    layers = count // 3
    model, tokens = h_t.shape
    cores, _, _, even = shard_rows = landing.shape[1:5]
    main = math.prod(shard_rows)
    half_main = main // cores
    rest = model - main
    inner = heads * head_dim
    prefix = kc.shape[-1]
    wide = shard.shape[-1]
    remote_rest = Unit(torus, count, extra, landing_extra)

    def unit(u):
        return Unit(torus, u, shard.at[u], landing.at[u])

    def push(u):
        unit(u).relay_block()

        @pl.when(u + 1 < count)
        def _():
            unit(u + 1).send_block()

        @pl.when(u + 3 < count)
        def _():
            unit(u + 3).send_own()

    def finish(u):
        unit(u).last_block()

        @pl.when(u + 2 < count)
        def _():
            unit(u + 2).relay_own()

        unit(u).complete()

    remote_rest.send_own()
    unit(0).send_own()
    unit(1).send_own()
    remote_rest.relay_own()
    unit(0).relay_own()
    remote_rest.send_block()
    remote_rest.relay_block()
    unit(0).send_block()
    unit(2).send_own()

    h_t[...] = hidden[...]
    o_t[pl.ds(0, LANES // 2), :] = jnp.zeros((LANES // 2, tokens), BF16)

    remote_rest.last_block()
    unit(1).relay_own()
    remote_rest.complete()

    def rest_copy(u):
        return pltpu.make_async_copy(landing_extra.at[:, :, :, u], raw, raw_sem)

    def spread(u, carry):
        rest_copy(u).start()
        rest_copy(u).wait()
        for i in range(cores):
            for j in range(side):
                for k in range(side):
                    at = ((i * side + j) * side + k) * raw.shape[3]
                    w_rest[u, at:at + raw.shape[3], :] = raw[i, j, k]
        return carry

    lax.fori_loop(0, count, spread, 0)
    push(0)
    finish(0)

    def w_copy(u, start, slot, size=TILE):
        return pltpu.make_async_copy(landing.at[u, :, :, :, :, pl.ds(start, size)],
                                     w_buf.at[slot, :, :, :, :, pl.ds(0, size)], w_sem.at[slot])

    def tiles(u, start_of, number, work):
        w_copy(u, start_of(0), 0).start()

        def turn(i, carry):
            slot = lax.rem(i, 2)

            @pl.when(i + 1 < number)
            def _():
                w_copy(u, start_of(i + 1), 1 - slot).start()

            w_copy(u, start_of(i), slot).wait()
            work(slot, start_of(i))
            return carry

        lax.fori_loop(0, number, turn, 0)

    def norm_rows(which, layer):
        gain = gains[layer, 2 * which:2 * which + 1, :]
        shift = gains[layer, 2 * which + 1:2 * which + 2, :]

        def turn(i, carry):
            at = pl.ds(pl.multiple_of(i * LANES, LANES), LANES)
            rows = jnp.transpose(normalized(h_t[:, at]))
            a_ref[at, :] = (rows * gain + shift).astype(BF16)
            return carry

        lax.fori_loop(0, tokens // LANES, turn, 0)

    def by_columns(u, slot, start, store):
        def turn(i, carry):
            local = pl.multiple_of(i * CHUNK, CHUNK)
            at = pl.ds(pl.multiple_of(start + local, LANES), CHUNK)
            w = w_buf[slot, :, :, :, :, pl.ds(local, CHUNK)].reshape(main, CHUNK)
            store(at, dot(a_ref[:, :main], w) + dot(a_ref[:, main:], w_rest[u, :, at]))
            return carry

        lax.fori_loop(0, TILE // CHUNK, turn, 0)

    def column(lane):
        lanes = lax.broadcasted_iota(jnp.int32, sides.shape, 1)
        return jnp.sum(jnp.where(lanes == lane, sides[...], 0.0), axis=1, keepdims=True)

    def add_rows(at, value, bias):
        h_t[at, :] = (h_t[at, :].astype(F32) + (value + bias)).astype(BF16)

    out_start = (3 * inner) // LANES * LANES
    first = TILE
    second = wide - out_start - first

    def head(h, carry):
        def rows(base):
            return pl.ds(pl.multiple_of(base + h * head_dim, head_dim), head_dim)

        query = qkv_t[rows(0), :]
        keys = jnp.concatenate([kc[rows(0), :], qkv_t[rows(inner), :]], axis=1)
        values = jnp.concatenate([vc[rows(0), :], qkv_t[rows(2 * inner), :]], axis=1)
        for b in range(tokens // CHUNK):
            upto = prefix + (b + 1) * CHUNK
            scores = dot(keys[:, :upto], query[:, b * CHUNK:(b + 1) * CHUNK], ((0,), (0,))) * (head_dim ** -0.5)
            position = lax.broadcasted_iota(jnp.int32, (upto, CHUNK), 0) - (upto - CHUNK)
            token = lax.broadcasted_iota(jnp.int32, (upto, CHUNK), 1)
            scores = jnp.where(position <= token, scores, -1e30)
            weights = jnp.exp(scores - jnp.max(scores, axis=0, keepdims=True))
            probs = (weights * (1.0 / jnp.sum(weights, axis=0, keepdims=True))).astype(BF16)
            o_t[rows(LANES // 2), b * CHUNK:(b + 1) * CHUNK] = dot(values[:, :upto], probs).astype(BF16)
        return carry

    def layer_turn(layer, carry):
        u = 3 * layer
        cached = [pltpu.make_async_copy(src.at[layer], dst, cache_sem.at[i])
                  for i, (src, dst) in enumerate(((k_cache, kc), (v_cache, vc)))]
        for copy in cached:
            copy.start()
        norm_rows(0, layer)

        def store_qkv(at, value):
            qkv_t[at, :] = jnp.transpose((value + qkv_bias[layer, :, at]).astype(BF16))

        last = qkv_t.shape[0] - TILE
        tiles(u, lambda i: pl.multiple_of(jnp.minimum(i * TILE, last), LANES), pl.cdiv(qkv_t.shape[0], TILE),
              lambda slot, start: by_columns(u, slot, start, store_qkv))
        w_copy(u, out_start, 0).start()
        w_copy(u, out_start + first, 1, second).start()
        fresh = [pltpu.make_async_copy(qkv_t.at[pl.ds((i + 1) * inner, inner), :], dst.at[layer], kv_sem.at[i])
                 for i, dst in enumerate((k_out, v_out))]
        for copy in fresh:
            copy.start()
        for copy in cached:
            copy.wait()
        early = heads // 2
        lax.fori_loop(0, early, head, 0)
        push(u + 1)
        lax.fori_loop(early, heads, head, 0)
        w_copy(u, out_start, 0).wait()
        w_copy(u, out_start + first, 1, second).wait()
        bias = column(2 * layer)
        for i in range(cores):
            at = slice(i * half_main, (i + 1) * half_main)
            value = dot(w_buf[0, i].reshape(half_main, TILE), o_t[:first, :])
            value += dot(w_buf[1, i, :, :, :, :second].reshape(half_main, second), o_t[first:, :])
            add_rows(at, value, bias[at])
        add_rows(slice(main, model), dot(w_rest[u, :, out_start:], o_t[...]), bias[main:])
        norm_rows(1, layer)
        for copy in fresh:
            copy.wait()

        finish(u + 1)

        def store_up(at, value):
            u_ref[:, at] = jax.nn.gelu(value + up_bias[layer, :, at], approximate=True).astype(BF16)

        tiles(u + 1, lambda i: pl.multiple_of(i * TILE, LANES), wide // TILE,
              lambda slot, start: by_columns(u + 1, slot, start, store_up))

        push(u + 2)
        finish(u + 2)
        acc[...] = jnp.zeros_like(acc)

        def down(slot, start):
            at = pl.ds(start, TILE)
            part = u_ref[:, at]
            for i in range(cores):
                acc[i * half_main:(i + 1) * half_main, :] += dot(w_buf[slot, i].reshape(half_main, TILE), part, ((1,), (1,)))
            acc[main:, :] += dot(w_rest[u + 2, :, at], part, ((1,), (1,)))

        tiles(u + 2, lambda i: pl.multiple_of(i * TILE, LANES), wide // TILE, down)
        add_rows(slice(None), acc[...], column(2 * layer + 1))

        @pl.when(layer + 1 < layers)
        def _():
            push(u + 3)
            finish(u + 3)

        return carry

    lax.fori_loop(0, layers, layer_turn, 0)
    gain, shift = column(2 * layers), column(2 * layers + 1)
    for i in range(tokens // LANES):
        at = slice(i * LANES, (i + 1) * LANES)
        out[:, at] = (normalized(h_t[:, at]) * gain + shift).astype(BF16)

    remote_rest.drain()

    def drain(u, carry):
        unit(u).drain()
        return carry

    lax.fori_loop(0, count, drain, 0)


def solution(mesh):
    part_axis, group_axis = mesh.axis_names
    side = math.isqrt(mesh.shape[group_axis] // 2)
    seq_spec = P((part_axis, group_axis))
    cache_spec = P(None, (part_axis, group_axis))
    replicated = P()
    in_specs = (seq_spec, cache_spec, cache_spec, replicated, replicated, P(None, group_axis), replicated,
                P(None, None, None, group_axis), replicated, replicated, replicated, P(None, group_axis), replicated,
                P(None, None, group_axis), replicated, replicated, replicated)
    out_specs = (seq_spec, cache_spec, cache_spec)

    def local_program(hidden, k_cache, v_cache, attn_gain, attn_shift, qkv_weight, qkv_bias, out_weight, out_bias, mlp_gain, mlp_shift, up_weight, up_bias, down_weight, down_bias, final_gain, final_shift):
        layers, depth, wide = up_weight.shape
        heads, head_dim = out_weight.shape[1:3]
        inner = heads * head_dim
        tokens, model = hidden.shape[1:]
        prefix = k_cache.shape[2]
        even = depth // 16 * 16
        odd = depth - even
        main = even * 2 * side * side
        w_q = qkv_weight.reshape(layers, depth, 3 * inner)
        w_o = jnp.transpose(out_weight, (0, 3, 1, 2)).reshape(layers, depth, inner)
        w_d = jnp.swapaxes(down_weight, 1, 2)
        shards = jnp.stack([jnp.concatenate([w_q, w_o], axis=2), up_weight, w_d], axis=1)
        shards = shards.reshape(layers * 3, depth, wide)

        def ordered(v):
            v = jnp.moveaxis(v.reshape((side, side, 2, depth) + v.shape[1:]), 2, 0)
            return jnp.concatenate([v[:, :, :, :even].reshape((main,) + v.shape[4:]),
                                    v[:, :, :, even:].reshape((model - main,) + v.shape[4:])])

        def restored(v):
            a = v[:main].reshape((2, side, side, even) + v.shape[1:])
            b = v[main:].reshape((2, side, side, odd) + v.shape[1:])
            return jnp.moveaxis(jnp.concatenate([a, b], axis=3), 0, 2).reshape(v.shape)

        gains = ordered(jnp.transpose(jnp.stack([attn_gain, attn_shift, mlp_gain, mlp_shift]), (2, 1, 0)))
        gains = jnp.transpose(gains, (1, 2, 0))
        sides = [v for i in range(layers) for v in (out_bias[i], down_bias[i])] + [final_gain, final_shift]
        sides = ordered(jnp.stack(sides, axis=1))

        def features(cache):
            return jnp.transpose(cache[:, 0], (0, 2, 3, 1)).reshape(layers, inner, prefix)

        any_space = pl.BlockSpec(memory_space=pl.ANY)
        vmem = pl.BlockSpec(memory_space=pltpu.VMEM)
        qkv_rows = pl.cdiv(3 * inner, LANES) * LANES
        bias = jnp.pad(qkv_bias.reshape(layers, 1, 3 * inner), ((0, 0), (0, 0), (0, qkv_rows - 3 * inner)))
        count = 3 * layers
        new = jax.ShapeDtypeStruct((layers, inner, tokens), BF16)
        dma = pltpu.SemaphoreType.DMA
        out, k_new, v_new, _, _ = pl.pallas_call(
            functools.partial(prefill_kernel, group_axis, side, heads, head_dim),
            out_shape=(jax.ShapeDtypeStruct((model, tokens), BF16), new, new,
                       jax.ShapeDtypeStruct((count, 2, side, side, even, wide), BF16),
                       jax.ShapeDtypeStruct((2, side, side, count, odd, wide), BF16)),
            in_specs=[vmem, vmem, vmem, any_space, any_space, vmem, vmem, vmem, vmem],
            out_specs=(vmem, any_space, any_space, any_space, any_space),
            scratch_shapes=[
                pltpu.VMEM((model, tokens), BF16),
                pltpu.VMEM((tokens, model), BF16),
                pltpu.VMEM((qkv_rows, tokens), BF16),
                pltpu.VMEM((LANES // 2 + inner, tokens), BF16),
                pltpu.VMEM((tokens, wide), BF16),
                pltpu.VMEM((count, model - main, wide), BF16),
                pltpu.VMEM((2, 2, side, side, even, TILE), BF16),
                pltpu.VMEM((2, side, side, odd, wide), BF16),
                pltpu.VMEM((model, tokens), F32),
                pltpu.VMEM((inner, prefix), BF16),
                pltpu.VMEM((inner, prefix), BF16),
                dma((count + 1, 2, 12)), dma((count + 1, 2, 12)), dma((count + 1, 2)),
                dma((2,)), dma, dma((2,)), dma((2,)),
            ],
            compiler_params=pltpu.CompilerParams(collective_id=0, has_side_effects=True, vmem_limit_bytes=67043328),
        )(shards[:, :even], shards[:, even:], ordered(hidden[0].T), features(k_cache), features(v_cache), gains, bias,
          up_bias.reshape(layers, 1, wide), sides)

        def tokens_first(v):
            return jnp.transpose(v.reshape(layers, 1, heads, head_dim, tokens), (0, 1, 4, 2, 3))

        return restored(out).T[None], tokens_first(k_new), tokens_first(v_new)

    return jax.shard_map(local_program, mesh=mesh, in_specs=in_specs, out_specs=out_specs, check_vma=False)
```

```python
import functools
import math

import jax
import jax.numpy as jnp
from jax import lax
from jax.experimental import pallas as pl
from jax.experimental.pallas import tpu as pltpu
from jax.sharding import PartitionSpec as P

MESH = pl.DeviceIdType.MESH
LANES = 128


class Torus:
    def __init__(self, axis, side, send_sem, recv_sem, local_sem):
        me = lax.axis_index(axis)
        self.axis, self.side = axis, side
        self.core = lax.rem(me, 2)
        self.x = lax.rem(me // 2, side)
        self.y = me // (2 * side)
        self.send_sem, self.recv_sem, self.local_sem = send_sem, recv_sem, local_sem

    def coord(self, dim, k):
        return lax.rem((self.x if dim == "x" else self.y) + (k + self.side), self.side)

    def device(self, y, x, core):
        return {self.axis: (y * self.side + x) * 2 + core}

    def step(self, dim, k):
        if dim == "x":
            return self.device(self.y, self.coord("x", k), self.core)
        return self.device(self.coord("y", k), self.x, self.core)

    def partner(self):
        return self.device(self.y, self.x, 1 - self.core)

    def meet(self):
        barrier = pltpu.get_barrier_semaphore()
        peers = [self.step(dim, k) for dim in ("x", "y") for k in (1, -1)] + [self.partner()]
        for peer in peers:
            pl.semaphore_signal(barrier, inc=1, device_id=peer, device_id_type=MESH)
        pl.semaphore_wait(barrier, len(peers))


class Unit:
    def __init__(self, torus, index, shard, landing, parts=None):
        self.torus, self.index, self.shard, self.landing = torus, index, shard, landing
        half = shard.shape[-1] // LANES // 2 * LANES
        self.columns = (pl.ds(0, half), pl.ds(half, shard.shape[-1] - half))
        self.rank = len(shard.shape)
        self.parts = parts or (shard.shape[0],)

    def rows(self, part, third):
        base = 0 if part is None else sum(self.parts[:part])
        size = self.shard.shape[0] if part is None else self.parts[part]
        cut = size // 2
        return (pl.ds(base, size), pl.ds(base, cut), pl.ds(base + cut, size - cut))[third]

    def tail(self, t, part, third):
        return (self.rows(part, third),) + (slice(None),) * (self.rank - 2) + (self.columns[t],)

    def own(self, t):
        return self.shard.at[self.tail(t, None, 0)]

    def piece(self, t, k, third=0):
        torus = self.torus
        where = (torus.y, torus.coord("x", k)) if t == 0 else (torus.coord("y", k), torus.x)
        return self.landing.at[(torus.core,) + where + self.tail(t, None, third)]

    def block(self, t, k, part, third=0):
        torus = self.torus
        where = (torus.coord("y", k), slice(None)) if t == 0 else (slice(None), torus.coord("x", k))
        return self.landing.at[(torus.core,) + where + self.tail(t, part, third)]

    def copy(self, t, slot, part=0):
        torus = self.torus
        first, second = ("x", "y") if t == 0 else ("y", "x")
        source, target, device = {
            0: lambda: (self.own(t), self.piece(t, 0), torus.step(first, 1)),
            1: lambda: (self.own(t), self.piece(t, 0), torus.step(first, -1)),
            2: lambda: (self.piece(t, -1, 1), None, torus.step(first, 1)),
            3: lambda: (self.piece(t, 1, 2), None, torus.step(first, -1)),
            4: lambda: (self.block(t, 0, part), None, torus.step(second, 1)),
            5: lambda: (self.block(t, 0, part), None, torus.step(second, -1)),
            6: lambda: (self.block(t, -1, part, 1), None, torus.step(second, 1)),
            7: lambda: (self.block(t, 1, part, 2), None, torus.step(second, -1)),
            8: lambda: (self.block(t, 0, part), None, torus.partner()),
            9: lambda: (self.block(t, -1, part), None, torus.partner()),
            10: lambda: (self.block(t, 1, part), None, torus.partner()),
            11: lambda: (self.block(t, 2, part), None, torus.partner()),
        }[slot]()
        at = (self.index, t, slot)
        return pltpu.make_async_remote_copy(
            src_ref=source, dst_ref=source if target is None else target,
            send_sem=torus.send_sem.at[at], recv_sem=torus.recv_sem.at[at],
            device_id=device, device_id_type=MESH)

    def keep(self, t):
        return pltpu.make_async_copy(self.own(t), self.piece(t, 0), self.torus.local_sem.at[self.index, t])

    def start(self, *slots, part=0):
        for t in range(2):
            for slot in slots:
                self.copy(t, slot, part).start()

    def arrived(self, *slots, part=0):
        for t in range(2):
            for slot in slots:
                self.copy(t, slot, part).wait_recv()

    def send_own(self):
        self.start(0, 1)
        for t in range(2):
            self.keep(t).start()

    def relay_own(self):
        for t in range(2):
            for slot in (0, 1):
                self.copy(t, slot).wait_recv()
                self.copy(t, slot + 2).start()

    def send_block(self, part=0):
        if part == 0:
            for t in range(2):
                self.keep(t).wait()
            self.arrived(2, 3)
        self.start(4, 5, 8, part=part)

    def send_blocks(self):
        for part in range(len(self.parts)):
            self.send_block(part)

    def relay_block(self, part=0):
        for t in range(2):
            for slot in (4, 5):
                self.copy(t, slot, part).wait_recv()
                self.copy(t, slot + 2, part).start()
                self.copy(t, slot + 5, part).start()

    def last_block(self, part=0):
        self.arrived(6, 7, part=part)
        self.start(11, part=part)

    def complete(self, part=0):
        self.arrived(8, 9, 10, 11, part=part)

    def drain(self):
        for t in range(2):
            for slot in range(4):
                self.copy(t, slot).wait_send()
            for part in range(len(self.parts)):
                for slot in range(4, 12):
                    self.copy(t, slot, part).wait_send()


TILE = 1280
CHUNK = 256
F32 = jnp.float32
BF16 = jnp.bfloat16


def dot(a, b, dims=((1,), (0,))):
    return lax.dot_general(a, b, (dims, ((), ())), preferred_element_type=F32)


def normalized(block):
    wide = block.astype(F32)
    centered = wide - jnp.mean(wide, axis=0, keepdims=True)
    return centered * lax.rsqrt(jnp.mean(centered * centered, axis=0, keepdims=True) + 1e-5)


def prefill_kernel(axis, side, heads, head_dim, w_qkv, w_out, w_up, w_down, odd_rows, hidden, k_cache, v_cache,
                   vectors, qkv_bias, up_bias, out, k_out, v_out, landing, landing_extra,
                   shard, extra, packed, h_t, a_ref, qkv_t, o_t, u_ref, w_rest, w_buf, raw, acc, kc, vc, sides,
                   send_sem, recv_sem, local_sem, w_sem, raw_sem, cache_sem, kv_sem, fill_sem, pack_sem):
    torus = Torus(axis, side, send_sem, recv_sem, local_sem)
    count = shard.shape[0]
    layers = count // 3
    model, tokens = h_t.shape
    cores, _, _, even = shard_rows = landing.shape[1:5]
    main = math.prod(shard_rows)
    half_main = main // cores
    rest = model - main
    inner = heads * head_dim
    prefix = kc.shape[-1]
    wide = shard.shape[-1]
    remote_rest = Unit(torus, count, extra, landing_extra)

    def unit(layer, j):
        u = 3 * layer + j
        return Unit(torus, u, shard.at[u], landing.at[u])

    def exists(layer, j, work):
        if j < 3:
            work()
        else:
            pl.when(3 * layer + j < count)(work)

    def push(layer, j, part=0):
        unit(layer, j).relay_block(part)
        if part + 1 == len(unit(layer, j).parts):
            exists(layer, j + 3, lambda: unit(layer, j + 3).send_own())
            exists(layer, j + 1, lambda: unit(layer, j + 1).send_blocks())

    def finish(layer, j, part=0):
        unit(layer, j).last_block(part)
        if part == 0:
            exists(layer, j + 2, lambda: unit(layer, j + 2).relay_own())
        unit(layer, j).complete(part)

    fills = [pltpu.make_async_copy(src.at[i, pl.ds(0, even), :], shard.at[3 * i + k], fill_sem.at[2 * i + k - 1])
             for i in range(layers) for k, src in ((1, w_up), (2, w_down))]
    for copy in fills:
        copy.start()

    def pack(layer):
        blocks = 3 * heads
        sources = [pltpu.make_async_copy(w_qkv.at[layer], packed.at[pl.ds(0, blocks)], pack_sem.at[0]),
                   pltpu.make_async_copy(w_out.at[layer], packed.at[pl.ds(blocks, heads)], pack_sem.at[1])]
        for copy in sources:
            copy.start()
        for copy in sources:
            copy.wait()

        def turn(i, carry):
            at = pl.ds(pl.multiple_of(i * LANES, LANES), LANES)
            tile = jnp.concatenate([packed[2 * i], packed[2 * i + 1]], axis=1)
            shard[3 * layer, :, at] = tile[:even]
            extra[3 * layer, :, at] = tile[even:]
            return carry

        lax.fori_loop(0, wide // LANES, turn, 0)
        for k in (1, 2):
            extra[3 * layer + k] = odd_rows[2 * layer + k - 1]

    pack(0)
    torus.meet()
    unit(0, 0).send_own()
    for i in range(1, layers):
        pack(i)
    for copy in fills:
        copy.wait()
    remote_rest.send_own()
    unit(0, 1).send_own()
    unit(0, 0).relay_own()
    remote_rest.relay_own()
    unit(0, 0).send_blocks()
    unit(0, 1).relay_own()
    remote_rest.send_blocks()
    unit(0, 2).send_own()
    h_t[...] = hidden[...]
    o_t[pl.ds(0, LANES // 2), :] = jnp.zeros((LANES // 2, tokens), BF16)
    sides[...] = jnp.transpose(vectors[...])
    remote_rest.relay_block()
    push(0, 0)
    remote_rest.last_block()
    unit(0, 2).relay_own()
    remote_rest.complete()

    def rest_copy(u):
        return pltpu.make_async_copy(landing_extra.at[:, :, :, u], raw, raw_sem)

    def spread(u, carry):
        rest_copy(u).start()
        rest_copy(u).wait()
        for i in range(cores):
            for j in range(side):
                for k in range(side):
                    at = ((i * side + j) * side + k) * raw.shape[3]
                    w_rest[u, at:at + raw.shape[3], :] = raw[i, j, k]
        return carry

    lax.fori_loop(0, count, spread, 0)
    unit(0, 0).last_block()
    unit(0, 0).complete()

    def w_copy(u, start, slot, size=TILE, rows=(0, even)):
        at = pl.ds(*rows)
        return pltpu.make_async_copy(landing.at[u, :, :, :, at, pl.ds(start, size)],
                                     w_buf.at[slot, :, :, :, at, pl.ds(0, size)], w_sem.at[slot])

    def tiles(u, start_of, number, work, rows=(0, even)):
        w_copy(u, start_of(0), 0, rows=rows).start()

        def turn(i, carry):
            slot = lax.rem(i, 2)

            @pl.when(i + 1 < number)
            def _():
                w_copy(u, start_of(i + 1), 1 - slot, rows=rows).start()

            w_copy(u, start_of(i), slot, rows=rows).wait()
            work(slot, start_of(i))
            return carry

        lax.fori_loop(0, number, turn, 0)

    def norm_rows(which, layer):
        gain = vectors[pl.ds(2 * which * layers + layer, 1), :]
        shift = vectors[pl.ds((2 * which + 1) * layers + layer, 1), :]

        def turn(i, carry):
            at = pl.ds(pl.multiple_of(i * LANES, LANES), LANES)
            rows = jnp.transpose(normalized(h_t[:, at]))
            a_ref[at, :] = (rows * gain + shift).astype(BF16)
            return carry

        lax.fori_loop(0, tokens // LANES, turn, 0)

    def by_columns(u, slot, start, store):
        def turn(i, carry):
            local = pl.multiple_of(i * CHUNK, CHUNK)
            at = pl.ds(pl.multiple_of(start + local, LANES), CHUNK)
            w = w_buf[slot, :, :, :, :, pl.ds(local, CHUNK)].reshape(main, CHUNK)
            store(at, dot(a_ref[:, :main], w) + dot(a_ref[:, main:], w_rest[u, :, at]))
            return carry

        lax.fori_loop(0, TILE // CHUNK, turn, 0)

    def column(lane):
        lanes = lax.broadcasted_iota(jnp.int32, sides.shape, 1)
        return jnp.sum(jnp.where(lanes == lane, sides[...], 0.0), axis=1, keepdims=True)

    def add_rows(at, value, bias):
        h_t[at, :] = (h_t[at, :].astype(F32) + (value + bias)).astype(BF16)

    out_start = (3 * inner) // LANES * LANES
    first = TILE
    second = wide - out_start - first

    def head(h, carry):
        def rows(base):
            return pl.ds(pl.multiple_of(base + h * head_dim, head_dim), head_dim)

        query = qkv_t[rows(0), :]
        keys = jnp.concatenate([kc[rows(0), :], qkv_t[rows(inner), :]], axis=1)
        values = jnp.concatenate([vc[rows(0), :], qkv_t[rows(2 * inner), :]], axis=1)
        position = lax.broadcasted_iota(jnp.int32, (CHUNK, CHUNK), 0)
        token = lax.broadcasted_iota(jnp.int32, (CHUNK, CHUNK), 1)
        for b in range(tokens // CHUNK):
            upto = prefix + (b + 1) * CHUNK
            scores = dot(keys[:, :upto], query[:, b * CHUNK:(b + 1) * CHUNK], ((0,), (0,))) * (head_dim ** -0.5)
            diagonal = jnp.where(position <= token, scores[upto - CHUNK:], -1e30)
            scores = jnp.concatenate([scores[:upto - CHUNK], diagonal], axis=0)
            weights = jnp.exp(scores - jnp.max(scores, axis=0, keepdims=True))
            probs = (weights * (1.0 / jnp.sum(weights, axis=0, keepdims=True))).astype(BF16)
            o_t[rows(LANES // 2), b * CHUNK:(b + 1) * CHUNK] = dot(values[:, :upto], probs).astype(BF16)
        return carry

    def two_heads(i, carry):
        head(2 * i, carry)
        head(2 * i + 1, carry)
        return carry

    def layer_turn(layer, carry):
        u = 3 * layer
        cached = [pltpu.make_async_copy(src.at[layer], dst, cache_sem.at[i])
                  for i, (src, dst) in enumerate(((k_cache, kc), (v_cache, vc)))]
        for copy in cached:
            copy.start()
        norm_rows(0, layer)

        def store_qkv(at, value):
            qkv_t[at, :] = jnp.transpose((value + qkv_bias[pl.ds(layer, 1), at]).astype(BF16))

        last = qkv_t.shape[0] - TILE
        tiles(u, lambda i: pl.multiple_of(jnp.minimum(i * TILE, last), LANES), pl.cdiv(qkv_t.shape[0], TILE),
              lambda slot, start: by_columns(u, slot, start, store_qkv))
        w_copy(u, out_start, 0).start()
        w_copy(u, out_start + first, 1, second).start()
        fresh = [pltpu.make_async_copy(qkv_t.at[pl.ds((i + 1) * inner, inner), :], dst.at[layer], kv_sem.at[i])
                 for i, dst in enumerate((k_out, v_out))]
        for copy in fresh:
            copy.start()
        for copy in cached:
            copy.wait()
        early = heads // 4
        lax.fori_loop(0, early, two_heads, 0)
        push(layer, 1)
        lax.fori_loop(early, heads // 2, two_heads, 0)
        for i in range(heads // 2 * 2, heads):
            head(i, 0)
        w_copy(u, out_start, 0).wait()
        w_copy(u, out_start + first, 1, second).wait()
        bias = column(4 * layers + layer)
        for i in range(cores):
            at = slice(i * half_main, (i + 1) * half_main)
            value = dot(w_buf[0, i].reshape(half_main, TILE), o_t[:first, :])
            value += dot(w_buf[1, i, :, :, :, :second].reshape(half_main, second), o_t[first:, :])
            add_rows(at, value, bias[at])
        add_rows(slice(main, model), dot(w_rest[u, :, out_start:], o_t[...]), bias[main:])
        norm_rows(1, layer)
        for copy in fresh:
            copy.wait()

        finish(layer, 1)

        def store_up(at, value):
            u_ref[:, at] = jax.nn.gelu(value + up_bias[pl.ds(layer, 1), at], approximate=True).astype(BF16)

        tiles(u + 1, lambda i: pl.multiple_of(i * TILE, LANES), wide // TILE,
              lambda slot, start: by_columns(u + 1, slot, start, store_up))

        push(layer, 2)
        bias = column(5 * layers + layer)
        acc[...] = jnp.zeros_like(acc)
        finish(layer, 2)

        def down(slot, start):
            at = pl.ds(start, TILE)
            value = u_ref[:, at]
            for i in range(cores):
                w = w_buf[slot, i].reshape(half_main, TILE)
                acc[i * half_main:(i + 1) * half_main, :] += dot(w, value, ((1,), (1,)))
            acc[main:, :] += dot(w_rest[u + 2, :, at], value, ((1,), (1,)))

        tiles(u + 2, lambda i: pl.multiple_of(i * TILE, LANES), wide // TILE, down)
        add_rows(slice(None), acc[...], bias)

        @pl.when(layer + 1 < layers)
        def _():
            push(layer, 3)
            finish(layer, 3)

        return carry

    lax.fori_loop(0, layers, layer_turn, 0)
    gain, shift = column(6 * layers), column(6 * layers + 1)
    odd = rest // (cores * side * side)
    for part in range(tokens // LANES):
        lanes = slice(part * LANES, (part + 1) * LANES)
        value = (normalized(h_t[:, lanes]) * gain + shift).astype(BF16)
        for i in range(cores):
            for j in range(side * side):
                block = i * side * side + j
                at = (j * cores + i) * (even + odd)
                out[at:at + even, lanes] = value[block * even:(block + 1) * even]
                out[at + even:at + even + odd, lanes] = value[main + block * odd:main + (block + 1) * odd]

    remote_rest.drain()

    def drain(layer, carry):
        for j in range(3):
            unit(layer, j).drain()
        return carry

    lax.fori_loop(0, layers, drain, 0)


def solution(mesh):
    part_axis, group_axis = mesh.axis_names
    side = math.isqrt(mesh.shape[group_axis] // 2)
    seq_spec = P((part_axis, group_axis))
    cache_spec = P(None, (part_axis, group_axis))
    replicated = P()
    in_specs = (seq_spec, cache_spec, cache_spec, replicated, replicated, P(None, group_axis), replicated,
                P(None, None, None, group_axis), replicated, replicated, replicated, P(None, group_axis), replicated,
                P(None, None, group_axis), replicated, replicated, replicated)
    out_specs = (seq_spec, cache_spec, cache_spec)

    def local_program(hidden, k_cache, v_cache, attn_gain, attn_shift, qkv_weight, qkv_bias, out_weight, out_bias, mlp_gain, mlp_shift, up_weight, up_bias, down_weight, down_bias, final_gain, final_shift):
        layers, depth, wide = up_weight.shape
        heads, head_dim = out_weight.shape[1:3]
        inner = heads * head_dim
        tokens, model = hidden.shape[1:]
        prefix = k_cache.shape[2]
        even = depth // 16 * 16
        odd = depth - even
        main = even * 2 * side * side
        w_q = jnp.transpose(qkv_weight, (0, 2, 3, 1, 4)).reshape(layers, 3 * heads, depth, head_dim)
        w_o = jnp.transpose(out_weight, (0, 1, 3, 2))
        w_d = jnp.swapaxes(down_weight, 1, 2)
        odd_rows = jnp.stack([up_weight[:, even:], w_d[:, even:]], axis=1).reshape(2 * layers, odd, wide)

        def ordered(v):
            v = jnp.moveaxis(v.reshape((side, side, 2, depth) + v.shape[1:]), 2, 0)
            return jnp.concatenate([v[:, :, :, :even].reshape((main,) + v.shape[4:]),
                                    v[:, :, :, even:].reshape((model - main,) + v.shape[4:])])

        rows = [attn_gain, attn_shift, mlp_gain, mlp_shift, out_bias, down_bias, final_gain[None], final_shift[None]]
        rows += [jnp.zeros((-(6 * layers + 2) % 8, model), F32)]
        vectors = jnp.concatenate(rows).reshape(-1, side * side, 2, depth).swapaxes(1, 2)
        vectors = jnp.concatenate([vectors[..., :even].reshape(-1, main), vectors[..., even:].reshape(-1, model - main)], axis=1)

        def features(cache):
            return jnp.transpose(cache[:, 0], (0, 2, 3, 1)).reshape(layers, inner, prefix)

        any_space = pl.BlockSpec(memory_space=pl.ANY)
        vmem = pl.BlockSpec(memory_space=pltpu.VMEM)
        qkv_rows = pl.cdiv(3 * inner, LANES) * LANES
        bias = jnp.pad(qkv_bias.reshape(layers, 3 * inner), ((0, 0), (0, qkv_rows - 3 * inner)))
        count = 3 * layers
        new = jax.ShapeDtypeStruct((layers, inner, tokens), BF16)
        dma = pltpu.SemaphoreType.DMA
        out, k_new, v_new, _, _ = pl.pallas_call(
            functools.partial(prefill_kernel, group_axis, side, heads, head_dim),
            out_shape=(jax.ShapeDtypeStruct((model, tokens), BF16), new, new,
                       jax.ShapeDtypeStruct((count, 2, side, side, even, wide), BF16),
                       jax.ShapeDtypeStruct((2, side, side, count, odd, wide), BF16)),
            in_specs=[any_space] * 4 + [vmem, vmem, any_space, any_space, vmem, vmem, vmem],
            out_specs=(vmem, any_space, any_space, any_space, any_space),
            scratch_shapes=[
                pltpu.VMEM((count, even, wide), BF16),
                pltpu.VMEM((count, odd, wide), BF16),
                pltpu.VMEM((4 * heads, depth, head_dim), BF16),
                pltpu.VMEM((model, tokens), BF16),
                pltpu.VMEM((tokens, model), BF16),
                pltpu.VMEM((qkv_rows, tokens), BF16),
                pltpu.VMEM((LANES // 2 + inner, tokens), BF16),
                pltpu.VMEM((tokens, wide), BF16),
                pltpu.VMEM((count, model - main, wide), BF16),
                pltpu.VMEM((2, 2, side, side, even, TILE), BF16),
                pltpu.VMEM((2, side, side, odd, wide), BF16),
                pltpu.VMEM((model, tokens), F32),
                pltpu.VMEM((inner, prefix), BF16),
                pltpu.VMEM((inner, prefix), BF16),
                pltpu.VMEM((model, vectors.shape[0]), F32),
                dma((count + 1, 2, 12)), dma((count + 1, 2, 12)), dma((count + 1, 2)),
                dma((2,)), dma, dma((2,)), dma((2,)), dma((2 * layers,)), dma((2,)),
            ],
            compiler_params=pltpu.CompilerParams(collective_id=0, has_side_effects=True, vmem_limit_bytes=67043328),
        )(w_q, w_o, up_weight, w_d, odd_rows, ordered(hidden[0].T), features(k_cache), features(v_cache), vectors, bias,
          up_bias)

        def tokens_first(v):
            return jnp.transpose(v.reshape(layers, 1, heads, head_dim, tokens), (0, 1, 4, 2, 3))

        return out.T[None], tokens_first(k_new), tokens_first(v_new)

    return jax.shard_map(local_program, mesh=mesh, in_specs=in_specs, out_specs=out_specs, check_vma=False)
```
